32 devices in a mesh: dp: 2 (over x), sp: 16 (over y, z, core).
Axes of the slice: x: 2, y: 2, z: 4, core: 2. Of those that a mesh axis runs over, the one named last changes fastest.
Arguments:
- x: bfloat16 [4096, 4096], P(('dp', 'sp')), parts along dimension 0
- gain: bfloat16 [4096], replicated
- wq: bfloat16 [4096, 4096], replicated
- wk: bfloat16 [4096, 256], replicated
- wv: bfloat16 [4096, 256], replicated
- wo: bfloat16 [4096, 4096], replicated
Outputs:
- output: bfloat16 [4096, 4096], P(('dp', 'sp')), parts along dimension 0
There are 2 independent parts. The reference program is written for one: setup_inputs(seed, part) draws one part's arguments, and reference() takes and returns one part's arrays. A program takes and returns all parts, laid end to end along the dimension named above; an argument that names none is the same for every part.
All inputs are finite; a program needn't handle non-finite values.
Results may differ from the reference program's by a relative error of at most 0.012.
Values are sent between devices in bfloat16 or wider.
A program may use at most 2 GiB of HBM per device.

```python
import jax
import jax.numpy as jnp
from jax import lax

ROWS = 2048
D = 4096
HEADS = 32
KV_HEADS = 2
HEAD = 128
THETA = 10000


def setup_inputs(seed: int = 0, part: int = 0) -> dict:
    kx, kn, kq, kk, kv, ko = jax.random.split(jax.random.key(seed), 6)

    def weights(key, rows, columns):
        return jax.random.normal(key, (rows, columns), jnp.float32) * rows**-0.5

    drawn = {
        "x": jax.random.normal(jax.random.fold_in(kx, part), (ROWS, D), jnp.float32),
        "gain": 1 + 0.1 * jax.random.normal(kn, (D,), jnp.float32),
        "wq": 2 * weights(kq, D, HEADS * HEAD),
        "wk": 2 * weights(kk, D, KV_HEADS * HEAD),
        "wv": 4 * weights(kv, D, KV_HEADS * HEAD),
        "wo": weights(ko, HEADS * HEAD, D),
    }
    return {k: v.astype(jnp.bfloat16) for k, v in drawn.items()}


def normed(x, gain):
    wide = x.astype(jnp.float32)
    scale = lax.rsqrt(jnp.mean(wide * wide, -1, keepdims=True) + 1e-6)
    return (wide * scale * gain.astype(jnp.float32)).astype(jnp.bfloat16)


def turned(t, place, theta):
    half = t.shape[-1] // 2
    angle = place.astype(jnp.float32)[:, None] * theta ** (-jnp.arange(half, dtype=jnp.float32) / half)
    cos, sin = jnp.cos(angle)[:, None], jnp.sin(angle)[:, None]
    a, b = t[..., :half].astype(jnp.float32), t[..., half:].astype(jnp.float32)
    return jnp.concatenate([a * cos - b * sin, b * cos + a * sin], -1).astype(jnp.bfloat16)


def matmul(a, w):
    return jnp.dot(a, w, preferred_element_type=jnp.float32).astype(jnp.bfloat16)


def einsum(form, a, b):
    return jnp.einsum(form, a.astype(jnp.float32), b.astype(jnp.float32))


def attention(q, k, v):
    scores = einsum("tgsd,ugd->gstu", q, k) * q.shape[-1] ** -0.5
    token = jnp.arange(q.shape[0])
    scores = jnp.where(token[:, None] >= token, scores, -jnp.inf)
    weights = jax.nn.softmax(scores, -1).astype(jnp.bfloat16)
    return einsum("gstu,ugd->tgsd", weights, v).astype(jnp.bfloat16)


def reference(x, gain, wq, wk, wv, wo):
    a, place = normed(x, gain), jnp.arange(ROWS)
    q = turned(matmul(a, wq).reshape(ROWS, HEADS, HEAD), place, THETA).reshape(ROWS, KV_HEADS, -1, HEAD)
    k = turned(matmul(a, wk).reshape(ROWS, KV_HEADS, HEAD), place, THETA)
    v = matmul(a, wv).reshape(ROWS, KV_HEADS, HEAD)
    seen = attention(q, k, v).reshape(ROWS, HEADS * HEAD)
    return (x.astype(jnp.float32) + jnp.dot(seen, wo, preferred_element_type=jnp.float32)).astype(jnp.bfloat16)
```

```python
import functools

import jax
import jax.numpy as jnp
import numpy as np
from jax import lax
from jax.experimental import pallas as pl
from jax.experimental.pallas import tpu as pltpu
from jax.sharding import PartitionSpec as P

HEAD = 128
THETA = 10000
HIDDEN = -2e30
EXPONENT = HEAD**-0.5 * 1.4426950408889634
VMEM = 67_043_328
T = 128
KEYS = 512
STRIP = 512
WIDE = 512


def _dot(a, b):
    return jnp.dot(a, b, preferred_element_type=jnp.float32)


def tables(tokens):
    half = HEAD // 2
    rate = np.float32(THETA) ** (-np.arange(half, dtype=np.float32) / np.float32(half))
    angle = (np.arange(tokens, dtype=np.float32)[None, :] * rate[:, None].astype(np.float32)).astype(np.float32).astype(np.float64)
    return np.cos(angle).astype(np.float32), np.sin(angle).astype(np.float32)


def turned(t, cos, sin):
    half = HEAD // 2
    a, b = t[:half].astype(jnp.float32), t[half:].astype(jnp.float32)
    return jnp.concatenate([a * cos - b * sin, b * cos + a * sin], 0).astype(jnp.bfloat16)


def kernel(x_h, gain_h, wq_h, wk_h, wv_h, wo_h, cos_h, sin_h, out_h,
           xs, gain_v, wk_v, wv_v, wq_v, wo_v, cs, a_v, q_t, kv, stage, top_s, mix_s, seen, acc, yb,
           load, x_sem, kv_send, kv_recv, seen_send, seen_recv, y_send, y_recv, y_own, *, devices):
    d, dp = lax.axis_index("sp"), lax.axis_index("dp")
    c, e = d // 2, d % 2
    partner = c * 2 + 1 - e
    there = (dp, partner)
    n_q = wq_v.shape[0]
    half = wq_v.shape[0] * WIDE
    heads = half // HEAD
    cols = heads * 2 * T

    def remote(src, dst, send, recv, to):
        return pltpu.make_async_remote_copy(src_ref=src, dst_ref=dst, send_sem=send, recv_sem=recv, device_id=to,
                                            device_id_type=pl.DeviceIdType.MESH)

    def columns(n):
        return pl.ds(pl.multiple_of(e * half + n * WIDE, 128), WIDE)

    def place(i):
        return pl.ds(pl.multiple_of(i * T, 128), T)

    loads = [pltpu.make_async_copy(x_h, xs.at[0], load.at[0]), pltpu.make_async_copy(gain_h, gain_v, load.at[1]),
             pltpu.make_async_copy(wk_h, wk_v, load.at[2]), pltpu.make_async_copy(wv_h, wv_v, load.at[3]),
             pltpu.make_async_copy(cos_h.at[:, place(d)], cs.at[0, 0], load.at[4]),
             pltpu.make_async_copy(sin_h.at[:, place(d)], cs.at[0, 1], load.at[5]),
             pltpu.make_async_copy(cos_h.at[:, place(partner)], cs.at[1, 0], load.at[6]),
             pltpu.make_async_copy(sin_h.at[:, place(partner)], cs.at[1, 1], load.at[7])]
    load_q = [pltpu.make_async_copy(wq_h.at[:, columns(n)], wq_v.at[n], load.at[8 + n]) for n in range(n_q)]
    load_o = []
    for i, rows in enumerate((e, 1 - e)):
        for n in range(n_q):
            src = wo_h.at[pl.ds(pl.multiple_of(rows * half, 128), half), columns(n)]
            load_o.append(pltpu.make_async_copy(src, wo_v.at[i, n], load.at[8 + n_q + i * n_q + n]))
    for copy in loads + load_q:
        copy.start()

    barrier = pltpu.get_barrier_semaphore()
    for i in range(1, devices):
        pl.semaphore_signal(barrier, inc=1, device_id=(dp, lax.rem(d + i, devices)), device_id_type=pl.DeviceIdType.MESH)

    def norm(i):
        wide = xs[i].astype(jnp.float32)
        scale = lax.rsqrt(jnp.mean(wide * wide, -1, keepdims=True) + 1e-6)
        a_v[i] = (wide * scale * gain_v[...].astype(jnp.float32)[None, :]).astype(jnp.bfloat16)

    loads[0].wait()
    loads[1].wait()
    norm(0)
    for i in range(2, 8):
        loads[i].wait()
    k = _dot(a_v[0], wk_v[...]).astype(jnp.bfloat16)
    v = _dot(a_v[0], wv_v[...]).astype(jnp.bfloat16)
    for h in range(2):
        at = slice(h * HEAD, (h + 1) * HEAD)
        stage[h, 0] = turned(k[:, at].T, cs[0, 0], cs[0, 1]).T
        stage[h, 1] = v[:, at].T
    kv[d] = stage[e]

    @pl.when(e == 0)
    def _():
        @pl.when(c % 2 == 0)
        def _():
            kv[pl.ds(2 * c + 2, 2)] = jnp.zeros((2, 2, T, HEAD), jnp.bfloat16)

    @pl.when(e == 1)
    def _():
        @pl.when(c % 2 == 0)
        def _():
            kv[pl.ds(2 * c + 2, 2)] = jnp.zeros((2, 2, T, HEAD), jnp.bfloat16)

    pl.semaphore_wait(barrier, devices - 1)
    send_x = remote(xs.at[0], xs.at[1], x_sem.at[0], x_sem.at[1], there)
    send_x.start()

    def send_kv(t):
        return remote(stage.at[t % 2], kv.at[d], kv_send.at[t], kv_recv.at[d], (dp, t))

    def goes(t):
        return (t // 2 > c) | (t == partner)

    for t in range(devices):
        @pl.when(goes(t))
        def _():
            send_kv(t).start()

    def queries(i, n):
        q = _dot(a_v[i], wq_v[n]).astype(jnp.bfloat16)
        cos, sin = cs[i, 0], cs[i, 1]
        for h in range(WIDE // HEAD):
            at = (n * (WIDE // HEAD) + h) * 2 * T + i * T
            q_t[:, at : at + T] = turned(q[:, h * HEAD : (h + 1) * HEAD].T, cos, sin)

    for n in range(n_q):
        load_q[n].wait()
        if n == n_q - 2:
            for copy in load_o:
                copy.start()
        queries(0, n)
    send_x.wait_recv()
    norm(1)
    for n in range(n_q):
        queries(1, n)

    per = KEYS // T
    ones = jnp.ones((8, KEYS), jnp.bfloat16)

    def block(j, first):
        for i in range(per):
            b = per * j + i

            @pl.when((b // 2 < c) | (b == partner))
            def _():
                remote(kv.at[b], kv.at[b], kv_send.at[b], kv_recv.at[b], there).wait_recv()

        keys = kv[pl.ds(per * j, per), 0].reshape(KEYS, HEAD)
        values = jnp.concatenate([jnp.concatenate([kv[per * j + i, 1] for i in range(per)], axis=1), ones], axis=0)
        if first:
            token = lax.rem(lax.broadcasted_iota(jnp.int32, (1, STRIP), 1), 2 * T)
            token = jnp.where(token < T, d * T + token, partner * T + token - T)
            ok = lax.broadcasted_iota(jnp.int32, (KEYS, STRIP), 0) + j * KEYS <= token
        strips = list(range(0, cols, STRIP))
        scores = [_dot(keys, q_t[:, at : at + STRIP]) for at in strips]
        weights, keeps = [], []
        for at, s in zip(strips, scores):
            if first:
                s = jnp.where(ok, s, HIDDEN)
                top = s.max(axis=0, keepdims=True)
            else:
                old = top_s[:, at : at + STRIP]
                top = jnp.maximum(old, s.max(axis=0, keepdims=True))
                keeps.append(jnp.exp2((old - top) * EXPONENT))
            top_s[:, at : at + STRIP] = top
            weights.append(jnp.exp2((s - top) * EXPONENT).astype(jnp.bfloat16))
        for n, (at, p) in enumerate(zip(strips, weights)):
            new = _dot(values, p)
            mix_s[:, at : at + STRIP] = new if first else mix_s[:, at : at + STRIP] * keeps[n] + new

    last = c // 2
    block(last, True)
    lax.fori_loop(0, last, lambda i, _: block(last - 1 - i, False), None)

    sends = []
    for n in range(n_q):
        for at in range(n * WIDE * 2, (n + 1) * WIDE * 2, 2 * T):
            o = (mix_s[:HEAD, at : at + 2 * T] * (1 / mix_s[HEAD : HEAD + 1, at : at + 2 * T])).astype(jnp.bfloat16)
            seen[0, :, at // 2 : at // 2 + HEAD] = o.T
        here = slice(n * WIDE, (n + 1) * WIDE)
        for i in range(2):
            sends.append(remote(seen.at[0, i * T : (i + 1) * T, here], seen.at[1, (1 - i) * T : (2 - i) * T, here],
                                seen_send.at[2 * n + i], seen_recv.at[2 * n + i], there))
            sends[-1].start()

    for copy in load_o:
        copy.wait()
    for n in range(n_q):
        acc[:, n * WIDE : (n + 1) * WIDE] = _dot(seen[0], wo_v[0, n])
    for copy in sends:
        copy.wait()
    outs = []
    for n in range(n_q):
        here = slice(n * WIDE, (n + 1) * WIDE)
        y = acc[:, here] + _dot(seen[1], wo_v[1, n])
        for i in range(2):
            yb[i * T : (i + 1) * T, here] = (xs[i, :, columns(n)].astype(jnp.float32) + y[i * T : (i + 1) * T]).astype(jnp.bfloat16)
        outs.append(pltpu.make_async_copy(yb.at[:T, here], out_h.at[:, columns(n)], y_own.at[n]))
        outs.append(remote(yb.at[T:, here], out_h.at[:, columns(n)], y_send.at[n], y_recv.at[n], there))
        outs[-2].start()
        outs[-1].start()
    send_x.wait_send()
    for t in range(devices):
        @pl.when(goes(t))
        def _():
            send_kv(t).wait_send()
    for n in range(n_q):
        outs[2 * n].wait()
        outs[2 * n + 1].wait_send()
    for n in range(n_q):
        theirs = pl.ds(pl.multiple_of((1 - e) * half + n * WIDE, 128), WIDE)
        remote(yb.at[T:, n * WIDE : (n + 1) * WIDE], out_h.at[:, theirs], y_send.at[n], y_recv.at[n], there).wait_recv()


def solution(mesh):
    devices = mesh.shape["sp"]

    def step(x, gain, wq, wk, wv, wo):
        own, depth = x.shape
        half = wq.shape[1] // 2
        n_q = half // WIDE
        cols = half // HEAD * 2 * T
        cos, sin = (jnp.asarray(t) for t in tables(devices * own))
        bf, f32 = jnp.bfloat16, jnp.float32
        anywhere = pl.BlockSpec(memory_space=pl.ANY)
        dma = lambda n: pltpu.SemaphoreType.DMA((n,))
        scratch = [
            pltpu.VMEM((2, own, depth), bf),
            pltpu.VMEM((depth,), bf),
            pltpu.VMEM(wk.shape, bf), pltpu.VMEM(wv.shape, bf),
            pltpu.VMEM((n_q, depth, WIDE), bf),
            pltpu.VMEM((2, n_q, half, WIDE), bf),
            pltpu.VMEM((2, 2, HEAD // 2, own), f32),
            pltpu.VMEM((2, own, depth), bf),
            pltpu.VMEM((HEAD, cols), bf),
            pltpu.VMEM((devices, 2, own, HEAD), bf),
            pltpu.VMEM((2, 2, own, HEAD), bf),
            pltpu.VMEM((1, cols), f32), pltpu.VMEM((HEAD + 8, cols), f32),
            pltpu.VMEM((2, 2 * own, half), bf),
            pltpu.VMEM((2 * own, half), f32), pltpu.VMEM((2 * own, half), bf),
            dma(8 + 3 * n_q), dma(2), dma(devices), dma(devices), dma(2 * n_q), dma(2 * n_q), dma(n_q), dma(n_q), dma(n_q),
        ]
        return pl.pallas_call(
            functools.partial(kernel, devices=devices),
            out_shape=jax.ShapeDtypeStruct((own, wo.shape[1]), bf),
            in_specs=[anywhere] * 8,
            out_specs=anywhere,
            scratch_shapes=scratch,
            compiler_params=pltpu.CompilerParams(collective_id=0, has_side_effects=True, vmem_limit_bytes=VMEM),
            cost_estimate=pl.CostEstimate(flops=14 * 10**9, bytes_accessed=38 * 10**6, transcendentals=8 * 10**6),
        )(x, gain, wq, wk, wv, wo, cos, sin)

    tokens, whole = P(("dp", "sp"), None), P(None, None)
    return jax.shard_map(
        step,
        mesh=mesh,
        in_specs=(tokens, P(None), whole, whole, whole, whole),
        out_specs=tokens,
        check_vma=False,
    )
```

```python
import functools

import jax
import jax.numpy as jnp
import numpy as np
from jax import lax
from jax.experimental import pallas as pl
from jax.experimental.pallas import tpu as pltpu
from jax.sharding import PartitionSpec as P

HEAD = 128
THETA = 10000
HIDDEN = -2e30
EXPONENT = HEAD**-0.5 * 1.4426950408889634
VMEM = 62 * 2**20
T = 128
KEYS = 512
STRIP = 512
WIDE = 512

DIRECT = {0: (4, 2, 1), 1: (5, 2, 4), 2: (6, 3, 5, 4), 3: (7, 6, 5, 4), 4: (5, 6, 7), 5: (6, 7), 6: (7,)}
RELAY = ({2: ((1, (3, 6)), (0, (3, 6))), 3: ((2, (7,)),)}, {1: ((0, (5,)),), 3: ((1, (7,)), (0, (7,)))})


def _dot(a, b):
    return jnp.dot(a, b, preferred_element_type=jnp.float32)


def tables(tokens):
    half = HEAD // 2
    rate = np.float32(THETA) ** (-np.arange(half, dtype=np.float32) / np.float32(half))
    angle = (np.arange(tokens, dtype=np.float32)[None, :] * rate[:, None].astype(np.float32)).astype(np.float32).astype(np.float64)
    return np.cos(angle).astype(np.float32), np.sin(angle).astype(np.float32)


def turned(t, cos, sin):
    half = HEAD // 2
    a, b = t[:half].astype(jnp.float32), t[half:].astype(jnp.float32)
    return jnp.concatenate([a * cos - b * sin, b * cos + a * sin], 0).astype(jnp.bfloat16)


def kernel(x_h, gain_h, wq_h, wk_h, wv_h, wo_h, cos_h, sin_h, out_ref,
           xs, gain_v, wk_v, wv_v, wq_v, wo_v, cs, a_v, q_t, kv, stage, top_s, mix_s, seen,
           load, x_sem, kv_send, kv_recv, relay_send, seen_send, seen_recv, y_send, y_recv, *, devices):
    d, dp = lax.axis_index("sp"), lax.axis_index("dp")
    c, e = d // 2, d % 2
    partner = c * 2 + 1 - e
    there = (dp, partner)
    n_q = wq_v.shape[0]
    half = wq_v.shape[0] * WIDE
    heads = half // HEAD
    cols = heads * 2 * T

    def remote(src, dst, send, recv, to):
        return pltpu.make_async_remote_copy(src_ref=src, dst_ref=dst, send_sem=send, recv_sem=recv, device_id=to,
                                            device_id_type=pl.DeviceIdType.MESH)

    def columns(n):
        return pl.ds(pl.multiple_of(e * half + n * WIDE, 128), WIDE)

    def place(i):
        return pl.ds(pl.multiple_of(i * T, 128), T)

    loads = [pltpu.make_async_copy(x_h, xs.at[0], load.at[0]), pltpu.make_async_copy(gain_h, gain_v, load.at[1]),
             pltpu.make_async_copy(wk_h, wk_v, load.at[2]), pltpu.make_async_copy(wv_h, wv_v, load.at[3]),
             pltpu.make_async_copy(cos_h.at[:, place(d)], cs.at[0, 0], load.at[4]),
             pltpu.make_async_copy(sin_h.at[:, place(d)], cs.at[0, 1], load.at[5]),
             pltpu.make_async_copy(cos_h.at[:, place(partner)], cs.at[1, 0], load.at[6]),
             pltpu.make_async_copy(sin_h.at[:, place(partner)], cs.at[1, 1], load.at[7])]
    load_q = [pltpu.make_async_copy(wq_h.at[:, columns(n)], wq_v.at[n], load.at[8 + n]) for n in range(n_q)]
    load_o = []
    for i, rows in enumerate((e, 1 - e)):
        for n in range(n_q):
            src = wo_h.at[pl.ds(pl.multiple_of(rows * half, 128), half), columns(n)]
            load_o.append(pltpu.make_async_copy(src, wo_v.at[i, n], load.at[8 + n_q + i * n_q + n]))
    for copy in loads + load_q:
        copy.start()

    barrier = pltpu.get_barrier_semaphore()
    for i in range(1, devices):
        pl.semaphore_signal(barrier, inc=1, device_id=(dp, lax.rem(d + i, devices)), device_id_type=pl.DeviceIdType.MESH)

    def norm(i):
        wide = xs[i].astype(jnp.float32)
        scale = lax.rsqrt(jnp.mean(wide * wide, -1, keepdims=True) + 1e-6)
        a_v[i] = (wide * scale * gain_v[...].astype(jnp.float32)[None, :]).astype(jnp.bfloat16)

    with jax.named_scope("wait_x"):
        loads[0].wait()
        loads[1].wait()
    with jax.named_scope("norm"):
        norm(0)
    with jax.named_scope("wait_kv_weights"):
        for i in range(2, 8):
            loads[i].wait()
    k = _dot(a_v[0], wk_v[...]).astype(jnp.bfloat16)
    v = _dot(a_v[0], wv_v[...]).astype(jnp.bfloat16)
    for h in range(2):
        at = slice(h * HEAD, (h + 1) * HEAD)
        stage[h, 0] = turned(k[:, at].T, cs[0, 0], cs[0, 1]).T
        stage[h, 1] = v[:, at].T
    kv[d] = stage[e]

    @pl.when(e == 0)
    def _():
        @pl.when(c % 2 == 0)
        def _():
            kv[pl.ds(2 * c + 2, 2)] = jnp.zeros((2, 2, T, HEAD), jnp.bfloat16)

    @pl.when(e == 1)
    def _():
        @pl.when(c % 2 == 0)
        def _():
            kv[pl.ds(2 * c + 2, 2)] = jnp.zeros((2, 2, T, HEAD), jnp.bfloat16)

    with jax.named_scope("wait_barrier"):
        pl.semaphore_wait(barrier, devices - 1)
    send_x = remote(xs.at[0], xs.at[1], x_sem.at[0], x_sem.at[1], there)
    send_x.start()

    def send_kv(t, h):
        return remote(stage.at[h], kv.at[d], kv_send.at[t], kv_recv.at[d], (dp, t))

    def own_blocks(act):
        act(send_kv(partner, 1 - e))
        for chip, to in DIRECT.items():
            @pl.when(c == chip)
            def _():
                for t in to:
                    for h in range(2):
                        act(send_kv(2 * t + h, h))

    def relays(part, act):
        for chip, blocks in RELAY[part].items():
            @pl.when(c == chip)
            def _():
                for b, to in blocks:
                    for i in (2 * b, 2 * b + 1):
                        for n, t in enumerate(to):
                            act(remote(kv.at[i], kv.at[i], relay_send.at[n, i], kv_recv.at[i], (dp, 2 * t + e)), n == 0)

    def relay(copy, first):
        if first:
            copy.wait_recv()
        copy.start()

    own_blocks(lambda copy: copy.start())

    def project(i, n):
        seen[0, i * T : (i + 1) * T, n * WIDE : (n + 1) * WIDE] = _dot(a_v[i], wq_v[n]).astype(jnp.bfloat16)

    def turn(i, n):
        for h in range(n * WIDE // HEAD, (n + 1) * WIDE // HEAD):
            raw = seen[0, i * T : (i + 1) * T, h * HEAD : (h + 1) * HEAD]
            q_t[:, h * 2 * T + i * T : h * 2 * T + (i + 1) * T] = turned(raw.T, cs[i, 0], cs[i, 1])

    with jax.named_scope("wait_wq"):
        load_q[0].wait()
    with jax.named_scope("q0"):
        project(0, 0)
    with jax.named_scope("wait_wq"):
        load_q[1].wait()
    with jax.named_scope("q1"):
        project(0, 1)
        turn(0, 0)
    with jax.named_scope("wait_wq"):
        load_q[2].wait()
    for copy in load_o:
        copy.start()
    with jax.named_scope("wait_partner_x"):
        send_x.wait_recv()
    with jax.named_scope("q2"):
        project(0, 2)
        norm(1)
        turn(0, 1)
    with jax.named_scope("relay"):
        relays(0, relay)
    with jax.named_scope("q3"):
        for n in range(3):
            project(1, n)
        turn(0, 2)
        turn(1, 0)
    with jax.named_scope("wait_wq"):
        load_q[3].wait()
    with jax.named_scope("q4"):
        for i in range(2):
            project(i, 3)
        for n in range(1, 3):
            turn(1, n)
    with jax.named_scope("relay"):
        relays(1, relay)

    per = KEYS // T
    ones = jnp.ones((8, KEYS), jnp.bfloat16)

    def block(j, first):
        with jax.named_scope("wait_keys"):
            for i in range(per):
                b = per * j + i

                @pl.when(((b // 2 < c) & (c > 3)) | (b == partner))
                def _():
                    remote(kv.at[b], kv.at[b], kv_send.at[b], kv_recv.at[b], there).wait_recv()

        with jax.named_scope("attend"):
            if first:
                for i in range(2):
                    turn(i, 3)
            attend(j, first)

    def attend(j, first):
        keys = kv[pl.ds(per * j, per), 0].reshape(KEYS, HEAD)
        values = jnp.concatenate([jnp.concatenate([kv[per * j + i, 1] for i in range(per)], axis=1), ones], axis=0)
        if first:
            token = lax.rem(lax.broadcasted_iota(jnp.int32, (1, STRIP), 1), 2 * T)
            token = jnp.where(token < T, d * T + token, partner * T + token - T)
            ok = lax.broadcasted_iota(jnp.int32, (KEYS, STRIP), 0) + j * KEYS <= token
        strips = list(range(0, cols, STRIP))
        scores = [_dot(keys, q_t[:, at : at + STRIP]) for at in strips]
        weights, keeps = [], []
        for at, s in zip(strips, scores):
            if first:
                s = jnp.where(ok, s, HIDDEN)
                top = s.max(axis=0, keepdims=True)
            else:
                old = top_s[:, at : at + STRIP]
                top = jnp.maximum(old, s.max(axis=0, keepdims=True))
                keeps.append(jnp.exp2((old - top) * EXPONENT))
            top_s[:, at : at + STRIP] = top
            weights.append(jnp.exp2((s - top) * EXPONENT).astype(jnp.bfloat16))
        for n, (at, p) in enumerate(zip(strips, weights)):
            new = _dot(values, p)
            mix_s[:, at : at + STRIP] = new if first else mix_s[:, at : at + STRIP] * keeps[n] + new

    last = c // 2
    block(last, True)

    def later(i, _):
        j = last - 1 - i
        block(jnp.where((c == 7) & (i < 2), 1 + i, jnp.where(c == 4, i, j)), False)

    lax.fori_loop(0, last, later, None)

    def send_y(n, core):
        to = pl.ds(pl.multiple_of(core * half + n * 2 * WIDE, 128), 2 * WIDE)
        return remote(a_v.at[1, :, 2 * n * WIDE : 2 * (n + 1) * WIDE], out_ref.at[:, to], y_send.at[n], y_recv.at[n], there)

    sends = []
    scope = jax.named_scope("result")
    scope.__enter__()
    for n in range(n_q):
        for at in range(n * WIDE * 2, (n + 1) * WIDE * 2, 2 * T):
            o = (mix_s[:HEAD, at : at + 2 * T] * (1 / mix_s[HEAD : HEAD + 1, at : at + 2 * T])).astype(jnp.bfloat16)
            seen[0, :, at // 2 : at // 2 + HEAD] = o.T
        here = slice(n * WIDE, (n + 1) * WIDE)
        for i in range(2):
            sends.append(remote(seen.at[0, i * T : (i + 1) * T, here], seen.at[1, (1 - i) * T : (2 - i) * T, here],
                                seen_send.at[2 * n + i], seen_recv.at[2 * n + i], there))
            sends[-1].start()

    scope.__exit__(None, None, None)

    with jax.named_scope("wait_wo"):
        for copy in load_o:
            copy.wait()
    with jax.named_scope("out_own"):
        for n in range(n_q):
            y = _dot(seen[0], wo_v[0, n])
            for i in range(2):
                mix_s[:T, (2 * n + i) * WIDE : (2 * n + i + 1) * WIDE] = y[i * T : (i + 1) * T]
    with jax.named_scope("wait_seen"):
        for copy in sends:
            copy.wait()
    outs = []
    with jax.named_scope("out_other"):
        for i in (1, 0):
            for n in range(n_q):
                here = slice(n * WIDE, (n + 1) * WIDE)
                y = mix_s[:T, (2 * n + i) * WIDE : (2 * n + i + 1) * WIDE] + _dot(seen[1, i * T : (i + 1) * T], wo_v[1, n])
                y = (xs[i, :, columns(n)].astype(jnp.float32) + y).astype(jnp.bfloat16)
                if i == 0:
                    out_ref[:, columns(n)] = y
                else:
                    a_v[1, :, here] = y
                    if n % 2 == 1:
                        outs.append(send_y(n // 2, e))
                        outs[-1].start()
    scope = jax.named_scope("wait_end")
    scope.__enter__()
    send_x.wait_send()
    own_blocks(lambda copy: copy.wait_send())
    for part in range(2):
        relays(part, lambda copy, first: copy.wait_send())
    for n in range(n_q // 2):
        outs[n].wait_send()
        send_y(n, 1 - e).wait_recv()
    scope.__exit__(None, None, None)


def solution(mesh):
    devices = mesh.shape["sp"]

    def step(x, gain, wq, wk, wv, wo):
        own, depth = x.shape
        half = wq.shape[1] // 2
        n_q = half // WIDE
        cols = half // HEAD * 2 * T
        cos, sin = (jnp.asarray(t) for t in tables(devices * own))
        bf, f32 = jnp.bfloat16, jnp.float32
        anywhere = pl.BlockSpec(memory_space=pl.ANY)
        dma = lambda n: pltpu.SemaphoreType.DMA((n,))
        scratch = [
            pltpu.VMEM((2, own, depth), bf),
            pltpu.VMEM((depth,), bf),
            pltpu.VMEM(wk.shape, bf), pltpu.VMEM(wv.shape, bf),
            pltpu.VMEM((n_q, depth, WIDE), bf),
            pltpu.VMEM((2, n_q, half, WIDE), bf),
            pltpu.VMEM((2, 2, HEAD // 2, own), f32),
            pltpu.VMEM((2, own, depth), bf),
            pltpu.VMEM((HEAD, cols), bf),
            pltpu.VMEM((devices, 2, own, HEAD), bf),
            pltpu.VMEM((2, 2, own, HEAD), bf),
            pltpu.VMEM((1, cols), f32), pltpu.VMEM((HEAD + 8, cols), f32),
            pltpu.VMEM((2, 2 * own, half), bf),
            dma(8 + 3 * n_q), dma(2), dma(devices), dma(devices), pltpu.SemaphoreType.DMA((2, devices)), dma(2 * n_q), dma(2 * n_q), dma(n_q // 2), dma(n_q // 2),
        ]
        return pl.pallas_call(
            functools.partial(kernel, devices=devices),
            out_shape=pltpu.VMEM((own, wo.shape[1]), bf),
            in_specs=[anywhere] * 8,
            out_specs=pl.BlockSpec(memory_space=pltpu.VMEM),
            scratch_shapes=scratch,
            compiler_params=pltpu.CompilerParams(collective_id=0, has_side_effects=True, vmem_limit_bytes=VMEM),
            cost_estimate=pl.CostEstimate(flops=14 * 10**9, bytes_accessed=38 * 10**6, transcendentals=8 * 10**6),
        )(x, gain, wq, wk, wv, wo, cos, sin)

    tokens, whole = P(("dp", "sp"), None), P(None, None)
    return jax.shard_map(
        step,
        mesh=mesh,
        in_specs=(tokens, P(None), whole, whole, whole, whole),
        out_specs=tokens,
        check_vma=False,
    )
```

```python
import functools

import jax
import jax.numpy as jnp
import numpy as np
from jax import lax
from jax.experimental import pallas as pl
from jax.experimental.pallas import tpu as pltpu
from jax.sharding import PartitionSpec as P

HEAD = 128
THETA = 10000
HIDDEN = -2e30
EXPONENT = HEAD**-0.5 * 1.4426950408889634
VMEM = 62 * 2**20
T = 128
KEYS = 512
STRIP = 512
WIDE = 512

DIRECT = {0: (4, 1, 2), 1: (5, 2, 4), 2: (6, 3, 5, 4), 3: (7, 6, 5, 4), 4: (5, 6, 7), 5: (6, 7), 6: (7,)}
RELAY = ({2: ((1, (3, 6)), (0, (3, 6))), 3: ((2, (7,)),)}, {1: ((0, (5,)),), 3: ((1, (7,)), (0, (7,)))})


def _dot(a, b):
    return jnp.dot(a, b, preferred_element_type=jnp.float32)


def tables(tokens):
    half = HEAD // 2
    rate = np.float32(THETA) ** (-np.arange(half, dtype=np.float32) / np.float32(half))
    angle = (np.arange(tokens, dtype=np.float32)[None, :] * rate[:, None].astype(np.float32)).astype(np.float32).astype(np.float64)
    return np.cos(angle).astype(np.float32), np.sin(angle).astype(np.float32)


def turned(t, cos, sin):
    half = HEAD // 2
    a, b = t[:half].astype(jnp.float32), t[half:].astype(jnp.float32)
    return jnp.concatenate([a * cos - b * sin, b * cos + a * sin], 0).astype(jnp.bfloat16)


def kernel(x_h, gain_h, wq_h, wk_h, wv_h, wo_h, cos_h, sin_h, out_ref,
           xs, gain_v, wk_v, wv_v, wq_v, wo_v, cs, a_v, q_t, kv, stage, top_s, mix_s, seen,
           load, x_sem, kv_send, kv_recv, relay_send, seen_send, seen_recv, y_send, y_recv, *, devices):
    d, dp = lax.axis_index("sp"), lax.axis_index("dp")
    c, e = d // 2, d % 2
    partner = c * 2 + 1 - e
    there = (dp, partner)
    n_q = wq_v.shape[0]
    half = wq_v.shape[0] * WIDE
    heads = half // HEAD
    cols = heads * 2 * T

    def remote(src, dst, send, recv, to):
        return pltpu.make_async_remote_copy(src_ref=src, dst_ref=dst, send_sem=send, recv_sem=recv, device_id=to,
                                            device_id_type=pl.DeviceIdType.MESH)

    def columns(n):
        return pl.ds(pl.multiple_of(e * half + n * WIDE, 128), WIDE)

    def place(i):
        return pl.ds(pl.multiple_of(i * T, 128), T)

    loads = [pltpu.make_async_copy(x_h, xs.at[0], load.at[0]), pltpu.make_async_copy(gain_h, gain_v, load.at[1]),
             pltpu.make_async_copy(wk_h, wk_v, load.at[2]), pltpu.make_async_copy(wv_h, wv_v, load.at[3]),
             pltpu.make_async_copy(cos_h.at[:, place(d)], cs.at[0, 0], load.at[4]),
             pltpu.make_async_copy(sin_h.at[:, place(d)], cs.at[0, 1], load.at[5]),
             pltpu.make_async_copy(cos_h.at[:, place(partner)], cs.at[1, 0], load.at[6]),
             pltpu.make_async_copy(sin_h.at[:, place(partner)], cs.at[1, 1], load.at[7])]
    load_q = [pltpu.make_async_copy(wq_h.at[:, columns(n)], wq_v.at[n], load.at[8 + n]) for n in range(n_q)]
    load_o = []
    for i, rows in enumerate((e, 1 - e)):
        for n in range(n_q):
            src = wo_h.at[pl.ds(pl.multiple_of(rows * half, 128), half), columns(n)]
            load_o.append(pltpu.make_async_copy(src, wo_v.at[i, n], load.at[8 + n_q + i * n_q + n]))
    for copy in loads + load_q:
        copy.start()

    barrier = pltpu.get_barrier_semaphore()
    for i in range(1, devices):
        pl.semaphore_signal(barrier, inc=1, device_id=(dp, lax.rem(d + i, devices)), device_id_type=pl.DeviceIdType.MESH)

    def norm(i):
        wide = xs[i].astype(jnp.float32)
        scale = lax.rsqrt(jnp.mean(wide * wide, -1, keepdims=True) + 1e-6)
        a_v[i] = (wide * scale * gain_v[...].astype(jnp.float32)[None, :]).astype(jnp.bfloat16)

    with jax.named_scope("wait_x"):
        loads[0].wait()
        loads[1].wait()
    with jax.named_scope("norm"):
        norm(0)
    send_x = remote(xs.at[0], xs.at[1], x_sem.at[0], x_sem.at[1], there)

    def enter(now):
        @pl.when(now)
        def _():
            with jax.named_scope("wait_barrier"):
                pl.semaphore_wait(barrier, devices - 1)
            send_x.start()

    enter(c > 4)
    with jax.named_scope("wait_kv_weights"):
        for i in range(2, 8):
            loads[i].wait()
    k = _dot(a_v[0], wk_v[...]).astype(jnp.bfloat16)
    v = _dot(a_v[0], wv_v[...]).astype(jnp.bfloat16)
    for h in range(2):
        at = slice(h * HEAD, (h + 1) * HEAD)
        stage[h, 0] = turned(k[:, at].T, cs[0, 0], cs[0, 1]).T
        stage[h, 1] = v[:, at].T
    kv[d] = stage[e]

    @pl.when(e == 0)
    def _():
        @pl.when(c % 2 == 0)
        def _():
            kv[pl.ds(2 * c + 2, 2)] = jnp.zeros((2, 2, T, HEAD), jnp.bfloat16)

    @pl.when(e == 1)
    def _():
        @pl.when(c % 2 == 0)
        def _():
            kv[pl.ds(2 * c + 2, 2)] = jnp.zeros((2, 2, T, HEAD), jnp.bfloat16)

    enter(c <= 4)

    def send_kv(t, h):
        return remote(stage.at[h], kv.at[d], kv_send.at[t], kv_recv.at[d], (dp, t))

    def own_blocks(act):
        act(send_kv(partner, 1 - e))
        for chip, to in DIRECT.items():
            @pl.when(c == chip)
            def _():
                for t in to:
                    for h in range(2):
                        act(send_kv(2 * t + h, h))

    def relays(part, act):
        for chip, blocks in RELAY[part].items():
            @pl.when(c == chip)
            def _():
                for b, to in blocks:
                    for i in (2 * b, 2 * b + 1):
                        for n, t in enumerate(to):
                            act(remote(kv.at[i], kv.at[i], relay_send.at[n, i], kv_recv.at[i], (dp, 2 * t + e)), n == 0)

    def relay(copy, first):
        if first:
            copy.wait_recv()
        copy.start()

    own_blocks(lambda copy: copy.start())

    def project(i, n):
        seen[0, i * T : (i + 1) * T, n * WIDE : (n + 1) * WIDE] = _dot(a_v[i], wq_v[n]).astype(jnp.bfloat16)

    def turn(i, n):
        for h in range(n * WIDE // HEAD, (n + 1) * WIDE // HEAD):
            raw = seen[0, i * T : (i + 1) * T, h * HEAD : (h + 1) * HEAD]
            q_t[:, h * 2 * T + i * T : h * 2 * T + (i + 1) * T] = turned(raw.T, cs[i, 0], cs[i, 1])

    with jax.named_scope("wait_wq"):
        load_q[0].wait()
    with jax.named_scope("q0"):
        project(0, 0)
    with jax.named_scope("wait_partner_x"):
        send_x.wait_recv()
    with jax.named_scope("norm"):
        norm(1)
        turn(0, 0)
    with jax.named_scope("wait_wq"):
        load_q[1].wait()
    with jax.named_scope("q1"):
        project(0, 1)
    with jax.named_scope("q2"):
        for n in range(2):
            project(1, n)
        turn(0, 1)
    with jax.named_scope("wait_wq"):
        load_q[2].wait()
    for copy in load_o:
        copy.start()
    with jax.named_scope("relay"):
        relays(0, relay)
    with jax.named_scope("q3"):
        for i in range(2):
            project(i, 2)
        for n in range(2):
            turn(1, n)
    with jax.named_scope("wait_wq"):
        load_q[3].wait()
    with jax.named_scope("q4"):
        for i in range(2):
            project(i, 3)
        for i in range(2):
            turn(i, 2)
    with jax.named_scope("relay"):
        relays(1, relay)

    per = KEYS // T
    ones = jnp.ones((8, KEYS), jnp.bfloat16)

    def block(j, first):
        with jax.named_scope("wait_keys"):
            for i in range(per):
                b = per * j + i

                @pl.when(((b // 2 < c) & (c > 3)) | (b == partner))
                def _():
                    remote(kv.at[b], kv.at[b], kv_send.at[b], kv_recv.at[b], there).wait_recv()

        with jax.named_scope("attend"):
            if first:
                for i in range(2):
                    turn(i, 3)
            attend(j, first)

    def attend(j, first):
        keys = kv[pl.ds(per * j, per), 0].reshape(KEYS, HEAD)
        values = jnp.concatenate([jnp.concatenate([kv[per * j + i, 1] for i in range(per)], axis=1), ones], axis=0)
        if first:
            token = lax.rem(lax.broadcasted_iota(jnp.int32, (1, STRIP), 1), 2 * T)
            token = jnp.where(token < T, d * T + token, partner * T + token - T)
            ok = lax.broadcasted_iota(jnp.int32, (KEYS, STRIP), 0) + j * KEYS <= token
        strips = list(range(0, cols, STRIP))
        scores = [_dot(keys, q_t[:, at : at + STRIP]) for at in strips]
        weights, keeps = [], []
        for at, s in zip(strips, scores):
            if first:
                s = jnp.where(ok, s, HIDDEN)
                top = s.max(axis=0, keepdims=True)
            else:
                old = top_s[:, at : at + STRIP]
                top = jnp.maximum(old, s.max(axis=0, keepdims=True))
                keeps.append(jnp.exp2((old - top) * EXPONENT))
            top_s[:, at : at + STRIP] = top
            weights.append(jnp.exp2((s - top) * EXPONENT).astype(jnp.bfloat16))
        for n, (at, p) in enumerate(zip(strips, weights)):
            new = _dot(values, p)
            mix_s[:, at : at + STRIP] = new if first else mix_s[:, at : at + STRIP] * keeps[n] + new

    last = c // 2
    block(last, True)

    def later(i, _):
        j = last - 1 - i
        block(jnp.where((c > 5) & (i < 2), 1 + i, jnp.where(c == 4, i, j)), False)

    lax.fori_loop(0, last, later, None)

    def send_y(n, core):
        to = pl.ds(pl.multiple_of(core * half + n * 2 * WIDE, 128), 2 * WIDE)
        return remote(a_v.at[1, :, 2 * n * WIDE : 2 * (n + 1) * WIDE], out_ref.at[:, to], y_send.at[n], y_recv.at[n], there)

    sends = []
    with jax.named_scope("wait_wo"):
        for copy in load_o:
            copy.wait()
    scope = jax.named_scope("result")
    scope.__enter__()
    for n in range(n_q):
        for at in range(n * WIDE * 2, (n + 1) * WIDE * 2, 2 * T):
            o = (mix_s[:HEAD, at : at + 2 * T] * (1 / mix_s[HEAD : HEAD + 1, at : at + 2 * T])).astype(jnp.bfloat16)
            seen[0, :, at // 2 : at // 2 + HEAD] = o.T
        here = slice(n * WIDE, (n + 1) * WIDE)
        for i in range(2):
            sends.append(remote(seen.at[0, i * T : (i + 1) * T, here], seen.at[1, (1 - i) * T : (2 - i) * T, here],
                                seen_send.at[2 * n + i], seen_recv.at[2 * n + i], there))
            sends[-1].start()


    for n in range(n_q):
        y = _dot(seen[0], wo_v[0, n])
        for i in range(2):
            mix_s[:T, (2 * n + i) * WIDE : (2 * n + i + 1) * WIDE] = y[i * T : (i + 1) * T]
    scope.__exit__(None, None, None)
    with jax.named_scope("wait_seen"):
        for copy in sends:
            copy.wait()
    outs = []
    with jax.named_scope("out_other"):
        for i in (1, 0):
            for n in range(n_q):
                here = slice(n * WIDE, (n + 1) * WIDE)
                y = mix_s[:T, (2 * n + i) * WIDE : (2 * n + i + 1) * WIDE] + _dot(seen[1, i * T : (i + 1) * T], wo_v[1, n])
                y = (xs[i, :, columns(n)].astype(jnp.float32) + y).astype(jnp.bfloat16)
                if i == 0:
                    out_ref[:, columns(n)] = y
                else:
                    a_v[1, :, here] = y
                    if n % 2 == 1:
                        outs.append(send_y(n // 2, e))
                        outs[-1].start()
    scope = jax.named_scope("wait_end")
    scope.__enter__()
    send_x.wait_send()
    own_blocks(lambda copy: copy.wait_send())
    for part in range(2):
        relays(part, lambda copy, first: copy.wait_send())
    for n in range(n_q // 2):
        outs[n].wait_send()
        send_y(n, 1 - e).wait_recv()
    scope.__exit__(None, None, None)


def solution(mesh):
    devices = mesh.shape["sp"]

    def step(x, gain, wq, wk, wv, wo):
        own, depth = x.shape
        half = wq.shape[1] // 2
        n_q = half // WIDE
        cols = half // HEAD * 2 * T
        cos, sin = (jnp.asarray(t) for t in tables(devices * own))
        bf, f32 = jnp.bfloat16, jnp.float32
        anywhere = pl.BlockSpec(memory_space=pl.ANY)
        dma = lambda n: pltpu.SemaphoreType.DMA((n,))
        scratch = [
            pltpu.VMEM((2, own, depth), bf),
            pltpu.VMEM((depth,), bf),
            pltpu.VMEM(wk.shape, bf), pltpu.VMEM(wv.shape, bf),
            pltpu.VMEM((n_q, depth, WIDE), bf),
            pltpu.VMEM((2, n_q, half, WIDE), bf),
            pltpu.VMEM((2, 2, HEAD // 2, own), f32),
            pltpu.VMEM((2, own, depth), bf),
            pltpu.VMEM((HEAD, cols), bf),
            pltpu.VMEM((devices, 2, own, HEAD), bf),
            pltpu.VMEM((2, 2, own, HEAD), bf),
            pltpu.VMEM((1, cols), f32), pltpu.VMEM((HEAD + 8, cols), f32),
            pltpu.VMEM((2, 2 * own, half), bf),
            dma(8 + 3 * n_q), dma(2), dma(devices), dma(devices), pltpu.SemaphoreType.DMA((2, devices)), dma(2 * n_q), dma(2 * n_q), dma(n_q // 2), dma(n_q // 2),
        ]
        return pl.pallas_call(
            functools.partial(kernel, devices=devices),
            out_shape=pltpu.VMEM((own, wo.shape[1]), bf),
            in_specs=[anywhere] * 8,
            out_specs=pl.BlockSpec(memory_space=pltpu.VMEM),
            scratch_shapes=scratch,
            compiler_params=pltpu.CompilerParams(collective_id=0, has_side_effects=True, vmem_limit_bytes=VMEM),
            cost_estimate=pl.CostEstimate(flops=14 * 10**9, bytes_accessed=38 * 10**6, transcendentals=8 * 10**6),
        )(x, gain, wq, wk, wv, wo, cos, sin)

    tokens, whole = P(("dp", "sp"), None), P(None, None)
    return jax.shard_map(
        step,
        mesh=mesh,
        in_specs=(tokens, P(None), whole, whole, whole, whole),
        out_specs=tokens,
        check_vma=False,
    )
```

```python
import functools

import jax
import jax.numpy as jnp
import numpy as np
from jax import lax
from jax.experimental import pallas as pl
from jax.experimental.pallas import tpu as pltpu
from jax.sharding import PartitionSpec as P

HEAD = 128
THETA = 10000
HIDDEN = -2e30
EXPONENT = HEAD**-0.5 * 1.4426950408889634
VMEM = 62 * 2**20
T = 128
KEYS = 512
STRIP = 512
WIDE = 512

DIRECT = {0: (1, 2, 4), 1: (2, 5, 4), 2: (3, 6), 3: (7, 6, 5, 4), 4: (5, 6, 7), 5: (6,), 6: (7,)}
FIRST = {0: 2, 1: 2, 2: 2, 3: 1, 4: 1, 5: 1, 6: 0}
RELAY = ({2: ((1, (3, 6)), (0, (3, 6))), 3: ((2, (7,)),)}, {1: ((0, (5,)),), 6: ((5, (7,)),)}, {3: ((1, (7,)),), 6: ((2, (4, 5)),)},
         {3: ((0, (7,)),)})


def _dot(a, b):
    return jnp.dot(a, b, preferred_element_type=jnp.float32)


def tables(tokens):
    half = HEAD // 2
    rate = np.float32(THETA) ** (-np.arange(half, dtype=np.float32) / np.float32(half))
    angle = (np.arange(tokens, dtype=np.float32)[None, :] * rate[:, None].astype(np.float32)).astype(np.float32).astype(np.float64)
    return np.cos(angle).astype(np.float32), np.sin(angle).astype(np.float32)


def turned(t, cos, sin):
    half = HEAD // 2
    a, b = t[:half].astype(jnp.float32), t[half:].astype(jnp.float32)
    return jnp.concatenate([a * cos - b * sin, b * cos + a * sin], 0).astype(jnp.bfloat16)


def kernel(x_h, gain_h, wq_h, wk_h, wv_h, wo_h, cos_h, sin_h, out_ref,
           xs, gain_v, wk_v, wv_v, wq_v, wo_v, cs, a_v, q_t, kv, stage, top_s, mix_s, seen,
           load, x_sem, kv_send, kv_recv, relay_send, seen_send, seen_recv, y_send, y_recv, *, devices):
    d, dp = lax.axis_index("sp"), lax.axis_index("dp")
    c, e = d // 2, d % 2
    partner = c * 2 + 1 - e
    there = (dp, partner)
    n_q = wq_v.shape[0]
    half = wq_v.shape[0] * WIDE
    heads = half // HEAD
    cols = heads * 2 * T

    def remote(src, dst, send, recv, to):
        return pltpu.make_async_remote_copy(src_ref=src, dst_ref=dst, send_sem=send, recv_sem=recv, device_id=to,
                                            device_id_type=pl.DeviceIdType.MESH)

    def columns(n):
        return pl.ds(pl.multiple_of(e * half + n * WIDE, 128), WIDE)

    def place(i):
        return pl.ds(pl.multiple_of(i * T, 128), T)

    loads = [pltpu.make_async_copy(x_h, xs.at[0], load.at[0]), pltpu.make_async_copy(gain_h, gain_v, load.at[1]),
             pltpu.make_async_copy(wk_h, wk_v, load.at[2]), pltpu.make_async_copy(wv_h, wv_v, load.at[3]),
             pltpu.make_async_copy(cos_h.at[:, place(d)], cs.at[0, 0], load.at[4]),
             pltpu.make_async_copy(sin_h.at[:, place(d)], cs.at[0, 1], load.at[5]),
             pltpu.make_async_copy(cos_h.at[:, place(partner)], cs.at[1, 0], load.at[6]),
             pltpu.make_async_copy(sin_h.at[:, place(partner)], cs.at[1, 1], load.at[7])]
    load_q = [pltpu.make_async_copy(wq_h.at[:, columns(n)], wq_v.at[n], load.at[8 + n]) for n in range(n_q)]
    load_o = []
    for i, rows in enumerate((e, 1 - e)):
        for n in range(n_q):
            src = wo_h.at[pl.ds(pl.multiple_of(rows * half, 128), half), columns(n)]
            load_o.append(pltpu.make_async_copy(src, wo_v.at[i, n], load.at[8 + n_q + i * n_q + n]))
    for copy in loads + load_q:
        copy.start()

    barrier = pltpu.get_barrier_semaphore()
    for i in range(1, devices):
        pl.semaphore_signal(barrier, inc=1, device_id=(dp, lax.rem(d + i, devices)), device_id_type=pl.DeviceIdType.MESH)

    def norm(i):
        wide = xs[i].astype(jnp.float32)
        scale = lax.rsqrt(jnp.mean(wide * wide, -1, keepdims=True) + 1e-6)
        a_v[i] = (wide * scale * gain_v[...].astype(jnp.float32)[None, :]).astype(jnp.bfloat16)

    with jax.named_scope("wait_x"):
        loads[0].wait()
        loads[1].wait()
    with jax.named_scope("norm"):
        norm(0)
    send_x = remote(xs.at[0], xs.at[1], x_sem.at[0], x_sem.at[1], there)

    def enter(now):
        @pl.when(now)
        def _():
            with jax.named_scope("wait_barrier"):
                pl.semaphore_wait(barrier, devices - 1)

    enter(c > 5)

    @pl.when(c > 5)
    def _():
        send_x.start()

    with jax.named_scope("wait_kv_weights"):
        for i in range(2, 8):
            loads[i].wait()
    k = _dot(a_v[0], wk_v[...]).astype(jnp.bfloat16)
    v = _dot(a_v[0], wv_v[...]).astype(jnp.bfloat16)
    for h in range(2):
        at = slice(h * HEAD, (h + 1) * HEAD)
        stage[h, 0] = turned(k[:, at].T, cs[0, 0], cs[0, 1]).T
        stage[h, 1] = v[:, at].T
    kv[d] = stage[e]

    enter(c <= 5)

    def send_kv(t, h):
        return remote(stage.at[h], kv.at[d], kv_send.at[t], kv_recv.at[d], (dp, t))

    def own_blocks(act, part):
        for chip, to in DIRECT.items():
            @pl.when(c == chip)
            def _():
                for t in to[FIRST[chip] :] if part else to[: FIRST[chip]]:
                    for h in range(2):
                        act(send_kv(2 * t + h, h))

    def relays(part, act):
        for chip, blocks in RELAY[part].items():
            @pl.when(c == chip)
            def _():
                for b, to in blocks:
                    for i in (2 * b, 2 * b + 1):
                        for n, t in enumerate(to):
                            act(remote(kv.at[i], kv.at[i], relay_send.at[n, i], kv_recv.at[i], (dp, 2 * t + e)), n == 0)

    def relay(copy, first):
        if first:
            copy.wait_recv()
        copy.start()

    own_blocks(lambda copy: copy.start(), 0)

    @pl.when(c <= 5)
    def _():
        send_x.start()

    send_kv(partner, 1 - e).start()
    own_blocks(lambda copy: copy.start(), 1)

    def project(i, n):
        seen[0, i * T : (i + 1) * T, n * WIDE : (n + 1) * WIDE] = _dot(a_v[i], wq_v[n]).astype(jnp.bfloat16)

    def project_both(n):
        q = _dot(a_v[...].reshape(2 * T, a_v.shape[2]), wq_v[n])
        seen[0, :, n * WIDE : (n + 1) * WIDE] = q.astype(jnp.bfloat16)

    def turn(i, n):
        for h in range(n * WIDE // HEAD, (n + 1) * WIDE // HEAD):
            raw = seen[0, i * T : (i + 1) * T, h * HEAD : (h + 1) * HEAD]
            q_t[:, h * 2 * T + i * T : h * 2 * T + (i + 1) * T] = turned(raw.T, cs[i, 0], cs[i, 1])

    with jax.named_scope("wait_wq"):
        load_q[0].wait()
    with jax.named_scope("q0"):
        project(0, 0)
    with jax.named_scope("wait_partner_x"):
        send_x.wait_recv()
    with jax.named_scope("norm"):
        norm(1)
        turn(0, 0)
    with jax.named_scope("wait_wq"):
        load_q[1].wait()
    with jax.named_scope("q1"):
        project_both(1)
    with jax.named_scope("q2"):
        project(1, 0)
        turn(0, 1)
    with jax.named_scope("wait_wq"):
        load_q[2].wait()
    for copy in load_o:
        copy.start()
    with jax.named_scope("relay"):
        relays(0, relay)
    with jax.named_scope("q3"):
        project_both(2)
        for n in range(2):
            turn(1, n)
    with jax.named_scope("relay"):
        relays(1, relay)
    with jax.named_scope("wait_wq"):
        load_q[3].wait()
    with jax.named_scope("q4"):
        project_both(3)
        for i in range(2):
            turn(i, 2)
    with jax.named_scope("relay"):
        relays(2, relay)

    per = KEYS // T

    def block(j, first):
        with jax.named_scope("wait_keys"):
            for i in range(per):
                b = per * j + i

                passed = (c <= 3) | ((c == 6) & ((b // 2 == 5) | (b // 2 == 2)))

                @pl.when(((b // 2 < c) & ~passed) | (b == partner))
                def _():
                    remote(kv.at[b], kv.at[b], kv_send.at[b], kv_recv.at[b], there).wait_recv()

        if not first:
            with jax.named_scope("attend"):
                attend(j, KEYS, 0)

    def attend(j, size, own):
        first = own > 0
        if first:
            for i in range(2):
                turn(i, 3)
            token = lax.rem(lax.broadcasted_iota(jnp.int32, (1, STRIP), 1), 2 * T)
            token = jnp.where(token < T, d * T + token, partner * T + token - T)
            ok = lax.broadcasted_iota(jnp.int32, (own, STRIP), 0) + c * 2 * T <= token
        n_b = size // T
        keys = kv[pl.ds(per * j, n_b), 0].reshape(size, HEAD)
        ones = jnp.ones((8, size), jnp.bfloat16)
        values = jnp.concatenate([jnp.concatenate([kv[per * j + i, 1] for i in range(n_b)], axis=1), ones], axis=0)
        strips = list(range(0, cols, STRIP))
        scores = [_dot(keys, q_t[:, at : at + STRIP]) for at in strips]
        weights, keeps = [], []
        for at, s in zip(strips, scores):
            if first:
                hidden = jnp.where(ok, s[size - own :], HIDDEN)
                s = jnp.concatenate([s[: size - own], hidden], axis=0) if size > own else hidden
                top = s.max(axis=0, keepdims=True)
            else:
                old = top_s[:, at : at + STRIP]
                top = jnp.maximum(old, s.max(axis=0, keepdims=True))
                keeps.append(jnp.exp2((old - top) * EXPONENT))
            top_s[:, at : at + STRIP] = top
            weights.append(jnp.exp2((s - top) * EXPONENT).astype(jnp.bfloat16))
        for n, (at, p) in enumerate(zip(strips, weights)):
            new = _dot(values, p)
            mix_s[:, at : at + STRIP] = new if first else mix_s[:, at : at + STRIP] * keeps[n] + new

    last = c // 2
    block(last, True)
    for odd in range(2):
        @pl.when(c % 2 == odd)
        def _():
            with jax.named_scope("attend"):
                attend(last, (1 + odd) * 2 * T, 2 * T)


    with jax.named_scope("relay"):
        relays(3, relay)

    def later(i, _):
        j = last - 1 - i
        block(jnp.where((c > 5) & (i < 2), 1 + i, jnp.where((c == 4) | (c == 5), i, j)), False)

    lax.fori_loop(0, last, later, None)

    def send_y(n, core):
        to = pl.ds(pl.multiple_of(core * half + n * 2 * WIDE, 128), 2 * WIDE)
        return remote(a_v.at[1, :, 2 * n * WIDE : 2 * (n + 1) * WIDE], out_ref.at[:, to], y_send.at[n], y_recv.at[n], there)

    sends = []
    with jax.named_scope("wait_wo"):
        for copy in load_o:
            copy.wait()
    scope = jax.named_scope("result")
    scope.__enter__()
    for n in range(n_q):
        for at in range(n * WIDE * 2, (n + 1) * WIDE * 2, 2 * T):
            o = (mix_s[:HEAD, at : at + 2 * T] * (1 / mix_s[HEAD : HEAD + 1, at : at + 2 * T])).astype(jnp.bfloat16)
            seen[0, :, at // 2 : at // 2 + HEAD] = o.T
        here = slice(n * WIDE, (n + 1) * WIDE)
        for i in range(2):
            sends.append(remote(seen.at[0, i * T : (i + 1) * T, here], seen.at[1, (1 - i) * T : (2 - i) * T, here],
                                seen_send.at[2 * n + i], seen_recv.at[2 * n + i], there))
            sends[-1].start()


    for n in range(n_q):
        y = _dot(seen[0], wo_v[0, n])
        for i in range(2):
            mix_s[:T, (2 * n + i) * WIDE : (2 * n + i + 1) * WIDE] = y[i * T : (i + 1) * T]
    scope.__exit__(None, None, None)
    with jax.named_scope("wait_seen"):
        for copy in sends:
            copy.wait()
    outs = []
    with jax.named_scope("out_other"):
        for i in (1, 0):
            for n in range(n_q):
                here = slice(n * WIDE, (n + 1) * WIDE)
                y = mix_s[:T, (2 * n + i) * WIDE : (2 * n + i + 1) * WIDE] + _dot(seen[1, i * T : (i + 1) * T], wo_v[1, n])
                y = (xs[i, :, columns(n)].astype(jnp.float32) + y).astype(jnp.bfloat16)
                if i == 0:
                    out_ref[:, columns(n)] = y
                else:
                    a_v[1, :, here] = y
                    if n % 2 == 1:
                        outs.append(send_y(n // 2, e))
                        outs[-1].start()
    scope = jax.named_scope("wait_end")
    scope.__enter__()
    send_x.wait_send()
    send_kv(partner, 1 - e).wait_send()
    for part in range(2):
        own_blocks(lambda copy: copy.wait_send(), part)
    for part in range(4):
        relays(part, lambda copy, first: copy.wait_send())
    for n in range(n_q // 2):
        outs[n].wait_send()
        send_y(n, 1 - e).wait_recv()
    scope.__exit__(None, None, None)


def solution(mesh):
    devices = mesh.shape["sp"]

    def step(x, gain, wq, wk, wv, wo):
        own, depth = x.shape
        half = wq.shape[1] // 2
        n_q = half // WIDE
        cols = half // HEAD * 2 * T
        cos, sin = (jnp.asarray(t) for t in tables(devices * own))
        bf, f32 = jnp.bfloat16, jnp.float32
        anywhere = pl.BlockSpec(memory_space=pl.ANY)
        dma = lambda n: pltpu.SemaphoreType.DMA((n,))
        scratch = [
            pltpu.VMEM((2, own, depth), bf),
            pltpu.VMEM((depth,), bf),
            pltpu.VMEM(wk.shape, bf), pltpu.VMEM(wv.shape, bf),
            pltpu.VMEM((n_q, depth, WIDE), bf),
            pltpu.VMEM((2, n_q, half, WIDE), bf),
            pltpu.VMEM((2, 2, HEAD // 2, own), f32),
            pltpu.VMEM((2, own, depth), bf),
            pltpu.VMEM((HEAD, cols), bf),
            pltpu.VMEM((devices, 2, own, HEAD), bf),
            pltpu.VMEM((2, 2, own, HEAD), bf),
            pltpu.VMEM((1, cols), f32), pltpu.VMEM((HEAD + 8, cols), f32),
            pltpu.VMEM((2, 2 * own, half), bf),
            dma(8 + 3 * n_q), dma(2), dma(devices), dma(devices), pltpu.SemaphoreType.DMA((2, devices)), dma(2 * n_q), dma(2 * n_q), dma(n_q // 2), dma(n_q // 2),
        ]
        return pl.pallas_call(
            functools.partial(kernel, devices=devices),
            out_shape=pltpu.VMEM((own, wo.shape[1]), bf),
            in_specs=[anywhere] * 8,
            out_specs=pl.BlockSpec(memory_space=pltpu.VMEM),
            scratch_shapes=scratch,
            compiler_params=pltpu.CompilerParams(collective_id=0, has_side_effects=True, vmem_limit_bytes=VMEM),
            cost_estimate=pl.CostEstimate(flops=14 * 10**9, bytes_accessed=38 * 10**6, transcendentals=8 * 10**6),
        )(x, gain, wq, wk, wv, wo, cos, sin)

    tokens, whole = P(("dp", "sp"), None), P(None, None)
    return jax.shard_map(
        step,
        mesh=mesh,
        in_specs=(tokens, P(None), whole, whole, whole, whole),
        out_specs=tokens,
        check_vma=False,
    )
```

```python
import functools

import jax
import jax.numpy as jnp
import numpy as np
from jax import lax
from jax.experimental import pallas as pl
from jax.experimental.pallas import tpu as pltpu
from jax.sharding import PartitionSpec as P

HEAD = 128
THETA = 10000
HIDDEN = -2e30
EXPONENT = HEAD**-0.5 * 1.4426950408889634
VMEM = 62 * 2**20
T = 128
KEYS = 512
STRIP = 512
WIDE = 512

DIRECT = {0: (1, 2, 4), 1: (2, 5, 4), 2: (3, 6), 3: (7, 6, 5, 4), 4: (5, 6, 7), 5: (6,), 6: (7,)}
FIRST = {0: 2, 1: 2, 2: 2, 3: 1, 4: 1, 5: 1, 6: 0}
RELAY = ({2: ((1, (3, 6)), (0, (3, 6))), 3: ((2, (7,)),)}, {1: ((0, (5,)),), 6: ((5, (7,)),)}, {3: ((1, (7,)), (0, (7,))), 6: ((2, (4, 5)),)})


def _dot(a, b):
    return jnp.dot(a, b, preferred_element_type=jnp.float32)


def tables(tokens):
    half = HEAD // 2
    rate = np.float32(THETA) ** (-np.arange(half, dtype=np.float32) / np.float32(half))
    angle = (np.arange(tokens, dtype=np.float32)[None, :] * rate[:, None].astype(np.float32)).astype(np.float32).astype(np.float64)
    return np.cos(angle).astype(np.float32), np.sin(angle).astype(np.float32)


def turned(t, cos, sin):
    half = HEAD // 2
    a, b = t[:half].astype(jnp.float32), t[half:].astype(jnp.float32)
    return jnp.concatenate([a * cos - b * sin, b * cos + a * sin], 0).astype(jnp.bfloat16)


def kernel(x_h, gain_h, wq_h, wk_h, wv_h, wo_h, cos_h, sin_h, out_ref,
           xs, gain_v, wk_v, wv_v, wq_v, wo_v, cs, a_v, q_t, kv, stage, top_s, mix_s, seen,
           load, x_sem, kv_send, kv_recv, relay_send, seen_send, seen_recv, y_send, y_recv, *, devices):
    d, dp = lax.axis_index("sp"), lax.axis_index("dp")
    c, e = d // 2, d % 2
    partner = c * 2 + 1 - e
    there = (dp, partner)
    n_q = wq_v.shape[0]
    half = wq_v.shape[0] * WIDE
    heads = half // HEAD
    cols = heads * 2 * T

    def remote(src, dst, send, recv, to):
        return pltpu.make_async_remote_copy(src_ref=src, dst_ref=dst, send_sem=send, recv_sem=recv, device_id=to,
                                            device_id_type=pl.DeviceIdType.MESH)

    def columns(n):
        return pl.ds(pl.multiple_of(e * half + n * WIDE, 128), WIDE)

    def place(i):
        return pl.ds(pl.multiple_of(i * T, 128), T)

    loads = [pltpu.make_async_copy(x_h, xs.at[0], load.at[0]), pltpu.make_async_copy(gain_h, gain_v, load.at[1]),
             pltpu.make_async_copy(wk_h, wk_v, load.at[2]), pltpu.make_async_copy(wv_h, wv_v, load.at[3]),
             pltpu.make_async_copy(cos_h.at[:, place(d)], cs.at[0, 0], load.at[4]),
             pltpu.make_async_copy(sin_h.at[:, place(d)], cs.at[0, 1], load.at[5]),
             pltpu.make_async_copy(cos_h.at[:, place(partner)], cs.at[1, 0], load.at[6]),
             pltpu.make_async_copy(sin_h.at[:, place(partner)], cs.at[1, 1], load.at[7])]
    load_q = [pltpu.make_async_copy(wq_h.at[:, columns(n)], wq_v.at[n], load.at[8 + n]) for n in range(n_q)]
    load_o = []
    for i, rows in enumerate((e, 1 - e)):
        for n in range(n_q):
            src = wo_h.at[pl.ds(pl.multiple_of(rows * half, 128), half), columns(n)]
            load_o.append(pltpu.make_async_copy(src, wo_v.at[i, n], load.at[8 + n_q + i * n_q + n]))
    for copy in loads + load_q:
        copy.start()

    barrier = pltpu.get_barrier_semaphore()
    for i in range(1, devices):
        pl.semaphore_signal(barrier, inc=1, device_id=(dp, lax.rem(d + i, devices)), device_id_type=pl.DeviceIdType.MESH)

    def norm(i):
        wide = xs[i].astype(jnp.float32)
        scale = lax.rsqrt(jnp.mean(wide * wide, -1, keepdims=True) + 1e-6)
        a_v[i] = (wide * scale * gain_v[...].astype(jnp.float32)[None, :]).astype(jnp.bfloat16)

    with jax.named_scope("wait_x"):
        loads[0].wait()
        loads[1].wait()
    with jax.named_scope("norm"):
        norm(0)
    send_x = remote(xs.at[0], xs.at[1], x_sem.at[0], x_sem.at[1], there)

    def enter(now):
        @pl.when(now)
        def _():
            with jax.named_scope("wait_barrier"):
                pl.semaphore_wait(barrier, devices - 1)

    enter(c > 5)

    @pl.when(c > 5)
    def _():
        send_x.start()

    with jax.named_scope("wait_kv_weights"):
        for i in range(2, 8):
            loads[i].wait()
    k = _dot(a_v[0], wk_v[...]).astype(jnp.bfloat16)
    v = _dot(a_v[0], wv_v[...]).astype(jnp.bfloat16)
    for h in range(2):
        at = slice(h * HEAD, (h + 1) * HEAD)
        stage[h, 0] = turned(k[:, at].T, cs[0, 0], cs[0, 1]).T
        stage[h, 1] = v[:, at].T
    kv[d] = stage[e]

    enter(c <= 5)

    def send_kv(t, h):
        return remote(stage.at[h], kv.at[d], kv_send.at[t], kv_recv.at[d], (dp, t))

    def own_blocks(act, part):
        for chip, to in DIRECT.items():
            @pl.when(c == chip)
            def _():
                for t in to[FIRST[chip] :] if part else to[: FIRST[chip]]:
                    for h in range(2):
                        act(send_kv(2 * t + h, h))

    def relays(part, act):
        for chip, blocks in RELAY[part].items():
            @pl.when(c == chip)
            def _():
                for b, to in blocks:
                    for i in (2 * b, 2 * b + 1):
                        for n, t in enumerate(to):
                            act(remote(kv.at[i], kv.at[i], relay_send.at[n, i], kv_recv.at[i], (dp, 2 * t + e)), n == 0)

    def relay(copy, first):
        if first:
            copy.wait_recv()
        copy.start()

    own_blocks(lambda copy: copy.start(), 0)

    @pl.when(c <= 5)
    def _():
        send_x.start()

    send_kv(partner, 1 - e).start()
    own_blocks(lambda copy: copy.start(), 1)

    def project(i, n):
        seen[0, i * T : (i + 1) * T, n * WIDE : (n + 1) * WIDE] = _dot(a_v[i], wq_v[n]).astype(jnp.bfloat16)

    def project_both(n):
        q = _dot(a_v[...].reshape(2 * T, a_v.shape[2]), wq_v[n])
        seen[0, :, n * WIDE : (n + 1) * WIDE] = q.astype(jnp.bfloat16)

    def turn(i, n):
        for h in range(n * WIDE // HEAD, (n + 1) * WIDE // HEAD):
            raw = seen[0, i * T : (i + 1) * T, h * HEAD : (h + 1) * HEAD]
            q_t[:, h * 2 * T + i * T : h * 2 * T + (i + 1) * T] = turned(raw.T, cs[i, 0], cs[i, 1])

    with jax.named_scope("wait_wq"):
        load_q[0].wait()
    with jax.named_scope("q0"):
        project(0, 0)
    with jax.named_scope("wait_partner_x"):
        send_x.wait_recv()
    with jax.named_scope("norm"):
        norm(1)
        turn(0, 0)
    with jax.named_scope("wait_wq"):
        load_q[1].wait()
    with jax.named_scope("q1"):
        project_both(1)
    with jax.named_scope("q2"):
        project(1, 0)
        turn(0, 1)
    with jax.named_scope("wait_wq"):
        load_q[2].wait()
    for copy in load_o:
        copy.start()
    with jax.named_scope("relay"):
        relays(0, relay)
    with jax.named_scope("q3"):
        project_both(2)
        for n in range(2):
            turn(1, n)
    with jax.named_scope("relay"):
        relays(1, relay)
    with jax.named_scope("wait_wq"):
        load_q[3].wait()
    with jax.named_scope("q4"):
        project_both(3)
        for i in range(2):
            turn(i, 2)
    with jax.named_scope("relay"):
        relays(2, relay)

    per = KEYS // T

    def block(j, first):
        with jax.named_scope("wait_keys"):
            for i in range(per):
                b = per * j + i

                passed = (c <= 3) | ((c == 6) & ((b // 2 == 5) | (b // 2 == 2)))

                @pl.when(((b // 2 < c) & ~passed) | (b == partner))
                def _():
                    remote(kv.at[b], kv.at[b], kv_send.at[b], kv_recv.at[b], there).wait_recv()

        if not first:
            with jax.named_scope("attend"):
                attend(j, KEYS, 0)

    def attend(j, size, own):
        first = own > 0
        if first:
            for i in range(2):
                turn(i, 3)
            token = lax.rem(lax.broadcasted_iota(jnp.int32, (1, STRIP), 1), 2 * T)
            token = jnp.where(token < T, d * T + token, partner * T + token - T)
            ok = lax.broadcasted_iota(jnp.int32, (own, STRIP), 0) + c * 2 * T <= token
        n_b = size // T
        keys = kv[pl.ds(per * j, n_b), 0].reshape(size, HEAD)
        ones = jnp.ones((8, size), jnp.bfloat16)
        values = jnp.concatenate([jnp.concatenate([kv[per * j + i, 1] for i in range(n_b)], axis=1), ones], axis=0)
        strips = list(range(0, cols, STRIP))
        scores = [_dot(keys, q_t[:, at : at + STRIP]) for at in strips]
        weights, keeps = [], []
        for at, s in zip(strips, scores):
            if first:
                hidden = jnp.where(ok, s[size - own :], HIDDEN)
                s = jnp.concatenate([s[: size - own], hidden], axis=0) if size > own else hidden
                top = s.max(axis=0, keepdims=True)
            else:
                old = top_s[:, at : at + STRIP]
                top = jnp.maximum(old, s.max(axis=0, keepdims=True))
                keeps.append(jnp.exp2((old - top) * EXPONENT))
            top_s[:, at : at + STRIP] = top
            weights.append(jnp.exp2((s - top) * EXPONENT).astype(jnp.bfloat16))
        for n, (at, p) in enumerate(zip(strips, weights)):
            new = _dot(values, p)
            mix_s[:, at : at + STRIP] = new if first else mix_s[:, at : at + STRIP] * keeps[n] + new

    last = c // 2
    block(last, True)
    for odd in range(2):
        @pl.when(c % 2 == odd)
        def _():
            with jax.named_scope("attend"):
                attend(last, (1 + odd) * 2 * T, 2 * T)


    def later(i, _):
        j = last - 1 - i
        block(jnp.where((c > 5) & (i < 2), 1 + i, jnp.where((c == 4) | (c == 5), i, j)), False)

    lax.fori_loop(0, last, later, None)

    def send_y(n, core):
        to = pl.ds(pl.multiple_of(core * half + n * 2 * WIDE, 128), 2 * WIDE)
        return remote(a_v.at[1, :, 2 * n * WIDE : 2 * (n + 1) * WIDE], out_ref.at[:, to], y_send.at[n], y_recv.at[n], there)

    sends = []
    with jax.named_scope("wait_wo"):
        for copy in load_o:
            copy.wait()
    scope = jax.named_scope("result")
    scope.__enter__()
    for n in range(n_q):
        for at in range(n * WIDE * 2, (n + 1) * WIDE * 2, 2 * T):
            o = (mix_s[:HEAD, at : at + 2 * T] * (1 / mix_s[HEAD : HEAD + 1, at : at + 2 * T])).astype(jnp.bfloat16)
            seen[0, :, at // 2 : at // 2 + HEAD] = o.T
        here = slice(n * WIDE, (n + 1) * WIDE)
        for i in range(2):
            sends.append(remote(seen.at[0, i * T : (i + 1) * T, here], seen.at[1, (1 - i) * T : (2 - i) * T, here],
                                seen_send.at[2 * n + i], seen_recv.at[2 * n + i], there))
            sends[-1].start()


    for n in range(n_q):
        y = _dot(seen[0], wo_v[0, n])
        for i in range(2):
            mix_s[:T, (2 * n + i) * WIDE : (2 * n + i + 1) * WIDE] = y[i * T : (i + 1) * T]
    scope.__exit__(None, None, None)
    with jax.named_scope("wait_seen"):
        for copy in sends:
            copy.wait()
    outs = []
    with jax.named_scope("out_other"):
        for i in (1, 0):
            for n in range(n_q):
                here = slice(n * WIDE, (n + 1) * WIDE)
                y = mix_s[:T, (2 * n + i) * WIDE : (2 * n + i + 1) * WIDE] + _dot(seen[1, i * T : (i + 1) * T], wo_v[1, n])
                y = (xs[i, :, columns(n)].astype(jnp.float32) + y).astype(jnp.bfloat16)
                if i == 0:
                    out_ref[:, columns(n)] = y
                else:
                    a_v[1, :, here] = y
                    if n % 2 == 1:
                        outs.append(send_y(n // 2, e))
                        outs[-1].start()
    scope = jax.named_scope("wait_end")
    scope.__enter__()
    send_x.wait_send()
    send_kv(partner, 1 - e).wait_send()
    for part in range(2):
        own_blocks(lambda copy: copy.wait_send(), part)
    for part in range(3):
        relays(part, lambda copy, first: copy.wait_send())
    for n in range(n_q // 2):
        outs[n].wait_send()
        send_y(n, 1 - e).wait_recv()
    scope.__exit__(None, None, None)


def solution(mesh):
    devices = mesh.shape["sp"]

    def step(x, gain, wq, wk, wv, wo):
        own, depth = x.shape
        half = wq.shape[1] // 2
        n_q = half // WIDE
        cols = half // HEAD * 2 * T
        cos, sin = (jnp.asarray(t) for t in tables(devices * own))
        bf, f32 = jnp.bfloat16, jnp.float32
        anywhere = pl.BlockSpec(memory_space=pl.ANY)
        dma = lambda n: pltpu.SemaphoreType.DMA((n,))
        scratch = [
            pltpu.VMEM((2, own, depth), bf),
            pltpu.VMEM((depth,), bf),
            pltpu.VMEM(wk.shape, bf), pltpu.VMEM(wv.shape, bf),
            pltpu.VMEM((n_q, depth, WIDE), bf),
            pltpu.VMEM((2, n_q, half, WIDE), bf),
            pltpu.VMEM((2, 2, HEAD // 2, own), f32),
            pltpu.VMEM((2, own, depth), bf),
            pltpu.VMEM((HEAD, cols), bf),
            pltpu.VMEM((devices, 2, own, HEAD), bf),
            pltpu.VMEM((2, 2, own, HEAD), bf),
            pltpu.VMEM((1, cols), f32), pltpu.VMEM((HEAD + 8, cols), f32),
            pltpu.VMEM((2, 2 * own, half), bf),
            dma(8 + 3 * n_q), dma(2), dma(devices), dma(devices), pltpu.SemaphoreType.DMA((2, devices)), dma(2 * n_q), dma(2 * n_q), dma(n_q // 2), dma(n_q // 2),
        ]
        return pl.pallas_call(
            functools.partial(kernel, devices=devices),
            out_shape=pltpu.VMEM((own, wo.shape[1]), bf),
            in_specs=[anywhere] * 8,
            out_specs=pl.BlockSpec(memory_space=pltpu.VMEM),
            scratch_shapes=scratch,
            compiler_params=pltpu.CompilerParams(collective_id=0, has_side_effects=True, vmem_limit_bytes=VMEM),
            cost_estimate=pl.CostEstimate(flops=14 * 10**9, bytes_accessed=38 * 10**6, transcendentals=8 * 10**6),
        )(x, gain, wq, wk, wv, wo, cos, sin)

    tokens, whole = P(("dp", "sp"), None), P(None, None)
    return jax.shard_map(
        step,
        mesh=mesh,
        in_specs=(tokens, P(None), whole, whole, whole, whole),
        out_specs=tokens,
        check_vma=False,
    )
```

```python
import functools

import jax
import jax.numpy as jnp
import numpy as np
from jax import lax
from jax.experimental import pallas as pl
from jax.experimental.pallas import tpu as pltpu
from jax.sharding import PartitionSpec as P

HEAD = 128
THETA = 10000
HIDDEN = -2e30
EXPONENT = HEAD**-0.5 * 1.4426950408889634
VMEM = 62 * 2**20
T = 128
KEYS = 512
STRIP = 512
WIDE = 512

DIRECT = {0: (2, 1, 4), 1: (2, 5, 4), 2: (3, 6), 3: (7, 6, 5, 4), 4: (5, 6, 7), 5: (6,), 6: (7,)}
FIRST = {0: 2, 1: 2, 2: 2, 3: 1, 4: 1, 5: 1, 6: 0}
RELAY = ({2: ((1, (3, 6)), (0, (3, 6))), 3: ((2, (7,)),)}, {1: ((0, (5,)),), 6: ((5, (7,)),)}, {3: ((1, (7,)), (0, (7,))), 6: ((2, (4, 5)),)})


def _dot(a, b):
    return jnp.dot(a, b, preferred_element_type=jnp.float32)


def tables(tokens):
    half = HEAD // 2
    rate = np.float32(THETA) ** (-np.arange(half, dtype=np.float32) / np.float32(half))
    angle = (np.arange(tokens, dtype=np.float32)[None, :] * rate[:, None].astype(np.float32)).astype(np.float32).astype(np.float64)
    return np.cos(angle).astype(np.float32), np.sin(angle).astype(np.float32)


def turned(t, cos, sin):
    half = HEAD // 2
    a, b = t[:half].astype(jnp.float32), t[half:].astype(jnp.float32)
    return jnp.concatenate([a * cos - b * sin, b * cos + a * sin], 0).astype(jnp.bfloat16)


def kernel(x_h, gain_h, wq_h, wk_h, wv_h, wo_h, cos_h, sin_h, out_ref,
           xs, gain_v, wk_v, wv_v, wq_v, wo_v, cs, a_v, q_t, kv, stage, top_s, mix_s, seen,
           load, x_sem, kv_send, kv_recv, relay_send, seen_send, seen_recv, y_send, y_recv, *, devices):
    d, dp = lax.axis_index("sp"), lax.axis_index("dp")
    c, e = d // 2, d % 2
    partner = c * 2 + 1 - e
    there = (dp, partner)
    n_q = wq_v.shape[0]
    half = wq_v.shape[0] * WIDE
    heads = half // HEAD
    cols = heads * 2 * T

    def remote(src, dst, send, recv, to):
        return pltpu.make_async_remote_copy(src_ref=src, dst_ref=dst, send_sem=send, recv_sem=recv, device_id=to,
                                            device_id_type=pl.DeviceIdType.MESH)

    def columns(n):
        return pl.ds(pl.multiple_of(e * half + n * WIDE, 128), WIDE)

    def place(i):
        return pl.ds(pl.multiple_of(i * T, 128), T)

    loads = [pltpu.make_async_copy(x_h, xs.at[0], load.at[0]), pltpu.make_async_copy(gain_h, gain_v, load.at[1]),
             pltpu.make_async_copy(wk_h, wk_v, load.at[2]), pltpu.make_async_copy(wv_h, wv_v, load.at[3]),
             pltpu.make_async_copy(cos_h.at[:, place(d)], cs.at[0, 0], load.at[4]),
             pltpu.make_async_copy(sin_h.at[:, place(d)], cs.at[0, 1], load.at[5]),
             pltpu.make_async_copy(cos_h.at[:, place(partner)], cs.at[1, 0], load.at[6]),
             pltpu.make_async_copy(sin_h.at[:, place(partner)], cs.at[1, 1], load.at[7])]
    load_q = [pltpu.make_async_copy(wq_h.at[:, columns(n)], wq_v.at[n], load.at[8 + n]) for n in range(n_q)]
    load_o = []
    for i, rows in enumerate((e, 1 - e)):
        for n in range(n_q):
            src = wo_h.at[pl.ds(pl.multiple_of(rows * half, 128), half), columns(n)]
            load_o.append(pltpu.make_async_copy(src, wo_v.at[i, n], load.at[8 + n_q + i * n_q + n]))
    for copy in loads + load_q:
        copy.start()

    barrier = pltpu.get_barrier_semaphore()
    for i in range(1, devices):
        pl.semaphore_signal(barrier, inc=1, device_id=(dp, lax.rem(d + i, devices)), device_id_type=pl.DeviceIdType.MESH)

    def norm(i):
        wide = xs[i].astype(jnp.float32)
        scale = lax.rsqrt(jnp.mean(wide * wide, -1, keepdims=True) + 1e-6)
        a_v[i] = (wide * scale * gain_v[...].astype(jnp.float32)[None, :]).astype(jnp.bfloat16)

    with jax.named_scope("wait_x"):
        loads[0].wait()
        loads[1].wait()
    with jax.named_scope("norm"):
        norm(0)
    send_x = remote(xs.at[0], xs.at[1], x_sem.at[0], x_sem.at[1], there)

    def enter(now):
        @pl.when(now)
        def _():
            with jax.named_scope("wait_barrier"):
                pl.semaphore_wait(barrier, devices - 1)

    enter(c > 5)

    @pl.when(c > 5)
    def _():
        send_x.start()

    with jax.named_scope("wait_kv_weights"):
        for i in range(2, 8):
            loads[i].wait()
    k = _dot(a_v[0], wk_v[...]).astype(jnp.bfloat16)
    v = _dot(a_v[0], wv_v[...]).astype(jnp.bfloat16)
    for h in range(2):
        at = slice(h * HEAD, (h + 1) * HEAD)
        stage[h, 0] = turned(k[:, at].T, cs[0, 0], cs[0, 1]).T
        stage[h, 1] = v[:, at].T
    kv[d] = stage[e]

    enter(c <= 5)

    def send_kv(t, h):
        return remote(stage.at[h], kv.at[d], kv_send.at[t], kv_recv.at[d], (dp, t))

    def own_blocks(act, part):
        for chip, to in DIRECT.items():
            @pl.when(c == chip)
            def _():
                for t in to[FIRST[chip] :] if part else to[: FIRST[chip]]:
                    for h in range(2):
                        act(send_kv(2 * t + h, h))

    def relays(part, act):
        for chip, blocks in RELAY[part].items():
            @pl.when(c == chip)
            def _():
                for b, to in blocks:
                    for i in (2 * b, 2 * b + 1):
                        for n, t in enumerate(to):
                            act(remote(kv.at[i], kv.at[i], relay_send.at[n, i], kv_recv.at[i], (dp, 2 * t + e)), n == 0)

    def relay(copy, first):
        if first:
            copy.wait_recv()
        copy.start()

    own_blocks(lambda copy: copy.start(), 0)

    @pl.when(c <= 5)
    def _():
        send_x.start()

    send_kv(partner, 1 - e).start()
    own_blocks(lambda copy: copy.start(), 1)

    def project(i, n):
        seen[0, i * T : (i + 1) * T, n * WIDE : (n + 1) * WIDE] = _dot(a_v[i], wq_v[n]).astype(jnp.bfloat16)

    def project_both(n):
        q = _dot(a_v[...].reshape(2 * T, a_v.shape[2]), wq_v[n])
        seen[0, :, n * WIDE : (n + 1) * WIDE] = q.astype(jnp.bfloat16)

    def turn(i, n):
        for h in range(n * WIDE // HEAD, (n + 1) * WIDE // HEAD):
            raw = seen[0, i * T : (i + 1) * T, h * HEAD : (h + 1) * HEAD]
            q_t[:, h * 2 * T + i * T : h * 2 * T + (i + 1) * T] = turned(raw.T, cs[i, 0], cs[i, 1])

    with jax.named_scope("wait_wq"):
        load_q[0].wait()
    with jax.named_scope("q0"):
        project(0, 0)
    with jax.named_scope("wait_partner_x"):
        send_x.wait_recv()
    with jax.named_scope("norm"):
        norm(1)
        turn(0, 0)
    with jax.named_scope("wait_wq"):
        load_q[1].wait()
    with jax.named_scope("q1"):
        project_both(1)
    with jax.named_scope("q2"):
        project(1, 0)
        turn(0, 1)
    with jax.named_scope("wait_wq"):
        load_q[2].wait()
    for copy in load_o:
        copy.start()
    with jax.named_scope("relay"):
        relays(0, relay)
    with jax.named_scope("q3"):
        project_both(2)
        for n in range(2):
            turn(1, n)
    with jax.named_scope("relay"):
        relays(1, relay)
    with jax.named_scope("wait_wq"):
        load_q[3].wait()
    with jax.named_scope("q4"):
        project_both(3)
        for i in range(2):
            turn(i, 2)
    with jax.named_scope("relay"):
        relays(2, relay)

    per = KEYS // T

    def block(j, first):
        with jax.named_scope("wait_keys"):
            for i in range(per):
                b = per * j + i

                passed = (c <= 3) | ((c == 6) & ((b // 2 == 5) | (b // 2 == 2)))

                @pl.when(((b // 2 < c) & ~passed) | (b == partner))
                def _():
                    remote(kv.at[b], kv.at[b], kv_send.at[b], kv_recv.at[b], there).wait_recv()

        if not first:
            with jax.named_scope("attend"):
                attend(j, KEYS, 0)

    def attend(j, size, own):
        first = own > 0
        if first:
            for i in range(2):
                turn(i, 3)
            token = lax.rem(lax.broadcasted_iota(jnp.int32, (1, STRIP), 1), 2 * T)
            token = jnp.where(token < T, d * T + token, partner * T + token - T)
            ok = lax.broadcasted_iota(jnp.int32, (own, STRIP), 0) + c * 2 * T <= token
        n_b = size // T
        keys = kv[pl.ds(per * j, n_b), 0].reshape(size, HEAD)
        ones = jnp.ones((8, size), jnp.bfloat16)
        values = jnp.concatenate([jnp.concatenate([kv[per * j + i, 1] for i in range(n_b)], axis=1), ones], axis=0)
        strips = list(range(0, cols, STRIP))
        scores = [_dot(keys, q_t[:, at : at + STRIP]) for at in strips]
        weights, keeps = [], []
        for at, s in zip(strips, scores):
            if first:
                hidden = jnp.where(ok, s[size - own :], HIDDEN)
                s = jnp.concatenate([s[: size - own], hidden], axis=0) if size > own else hidden
                top = s.max(axis=0, keepdims=True)
            else:
                old = top_s[:, at : at + STRIP]
                top = jnp.maximum(old, s.max(axis=0, keepdims=True))
                keeps.append(jnp.exp2((old - top) * EXPONENT))
            top_s[:, at : at + STRIP] = top
            weights.append(jnp.exp2((s - top) * EXPONENT).astype(jnp.bfloat16))
        for n, (at, p) in enumerate(zip(strips, weights)):
            new = _dot(values, p)
            mix_s[:, at : at + STRIP] = new if first else mix_s[:, at : at + STRIP] * keeps[n] + new

    last = c // 2
    block(last, True)
    for odd in range(2):
        @pl.when(c % 2 == odd)
        def _():
            with jax.named_scope("attend"):
                attend(last, (1 + odd) * 2 * T, 2 * T)


    def later(i, _):
        j = last - 1 - i
        block(jnp.where((c > 5) & (i < 2), 1 + i, jnp.where((c == 4) | (c == 5), i, j)), False)

    lax.fori_loop(0, last, later, None)

    def send_y(n, core):
        to = pl.ds(pl.multiple_of(core * half + n * 2 * WIDE, 128), 2 * WIDE)
        return remote(a_v.at[1, :, 2 * n * WIDE : 2 * (n + 1) * WIDE], out_ref.at[:, to], y_send.at[n], y_recv.at[n], there)

    sends = []
    with jax.named_scope("wait_wo"):
        for copy in load_o:
            copy.wait()
    scope = jax.named_scope("result")
    scope.__enter__()
    for n in range(n_q):
        for at in range(n * WIDE * 2, (n + 1) * WIDE * 2, 2 * T):
            o = (mix_s[:HEAD, at : at + 2 * T] * (1 / mix_s[HEAD : HEAD + 1, at : at + 2 * T])).astype(jnp.bfloat16)
            seen[0, :, at // 2 : at // 2 + HEAD] = o.T
        here = slice(n * WIDE, (n + 1) * WIDE)
        for i in range(2):
            sends.append(remote(seen.at[0, i * T : (i + 1) * T, here], seen.at[1, (1 - i) * T : (2 - i) * T, here],
                                seen_send.at[2 * n + i], seen_recv.at[2 * n + i], there))
            sends[-1].start()


    for n in range(n_q):
        y = _dot(seen[0], wo_v[0, n])
        for i in range(2):
            mix_s[:T, (2 * n + i) * WIDE : (2 * n + i + 1) * WIDE] = y[i * T : (i + 1) * T]
    scope.__exit__(None, None, None)
    with jax.named_scope("wait_seen"):
        for copy in sends:
            copy.wait()
    outs = []
    with jax.named_scope("out_other"):
        for i in (1, 0):
            for n in range(n_q):
                here = slice(n * WIDE, (n + 1) * WIDE)
                y = mix_s[:T, (2 * n + i) * WIDE : (2 * n + i + 1) * WIDE] + _dot(seen[1, i * T : (i + 1) * T], wo_v[1, n])
                y = (xs[i, :, columns(n)].astype(jnp.float32) + y).astype(jnp.bfloat16)
                if i == 0:
                    out_ref[:, columns(n)] = y
                else:
                    a_v[1, :, here] = y
                    if n % 2 == 1:
                        outs.append(send_y(n // 2, e))
                        outs[-1].start()
    scope = jax.named_scope("wait_end")
    scope.__enter__()
    send_x.wait_send()
    send_kv(partner, 1 - e).wait_send()
    for part in range(2):
        own_blocks(lambda copy: copy.wait_send(), part)
    for part in range(3):
        relays(part, lambda copy, first: copy.wait_send())
    for n in range(n_q // 2):
        outs[n].wait_send()
        send_y(n, 1 - e).wait_recv()
    scope.__exit__(None, None, None)


def solution(mesh):
    devices = mesh.shape["sp"]

    def step(x, gain, wq, wk, wv, wo):
        own, depth = x.shape
        half = wq.shape[1] // 2
        n_q = half // WIDE
        cols = half // HEAD * 2 * T
        cos, sin = (jnp.asarray(t) for t in tables(devices * own))
        bf, f32 = jnp.bfloat16, jnp.float32
        anywhere = pl.BlockSpec(memory_space=pl.ANY)
        dma = lambda n: pltpu.SemaphoreType.DMA((n,))
        scratch = [
            pltpu.VMEM((2, own, depth), bf),
            pltpu.VMEM((depth,), bf),
            pltpu.VMEM(wk.shape, bf), pltpu.VMEM(wv.shape, bf),
            pltpu.VMEM((n_q, depth, WIDE), bf),
            pltpu.VMEM((2, n_q, half, WIDE), bf),
            pltpu.VMEM((2, 2, HEAD // 2, own), f32),
            pltpu.VMEM((2, own, depth), bf),
            pltpu.VMEM((HEAD, cols), bf),
            pltpu.VMEM((devices, 2, own, HEAD), bf),
            pltpu.VMEM((2, 2, own, HEAD), bf),
            pltpu.VMEM((1, cols), f32), pltpu.VMEM((HEAD + 8, cols), f32),
            pltpu.VMEM((2, 2 * own, half), bf),
            dma(8 + 3 * n_q), dma(2), dma(devices), dma(devices), pltpu.SemaphoreType.DMA((2, devices)), dma(2 * n_q), dma(2 * n_q), dma(n_q // 2), dma(n_q // 2),
        ]
        return pl.pallas_call(
            functools.partial(kernel, devices=devices),
            out_shape=pltpu.VMEM((own, wo.shape[1]), bf),
            in_specs=[anywhere] * 8,
            out_specs=pl.BlockSpec(memory_space=pltpu.VMEM),
            scratch_shapes=scratch,
            compiler_params=pltpu.CompilerParams(collective_id=0, has_side_effects=True, vmem_limit_bytes=VMEM),
            cost_estimate=pl.CostEstimate(flops=14 * 10**9, bytes_accessed=38 * 10**6, transcendentals=8 * 10**6),
        )(x, gain, wq, wk, wv, wo, cos, sin)

    tokens, whole = P(("dp", "sp"), None), P(None, None)
    return jax.shard_map(
        step,
        mesh=mesh,
        in_specs=(tokens, P(None), whole, whole, whole, whole),
        out_specs=tokens,
        check_vma=False,
    )
```
